32 devices in a mesh: groups: 2 (over x), expert: 16 (over z, y, core).
Axes of the slice: x: 2, y: 2, z: 4, core: 2. Of those that a mesh axis runs over, the one named last changes fastest.
Arguments:
- tokens: bfloat16 [1024, 2048], P(('groups', 'expert')), parts along dimension 0, may hold values from -6 to 6
- expert_ids: int32 [1024, 2], P(('groups', 'expert')), parts along dimension 0, may hold values from 0 to 7, all different within a row; in each aligned block of 32 rows (0 to 31, 32 to 63, ...) at most 16 rows name the same one
- member_ids: int32 [1024], P(('groups', 'expert')), parts along dimension 0, may hold values from 0 to 7
- combine_weights: float32 [1024, 2], P(('groups', 'expert')), parts along dimension 0, may hold values from 0.25 to 1
- gate_weight: bfloat16 [2048, 57344], P(None, 'expert'), may hold values from -0.125 to 0.125
- up_weight: bfloat16 [2048, 57344], P(None, 'expert'), may hold values from -0.125 to 0.125
- down_weight: bfloat16 [57344, 2048], P('expert'), may hold values from -0.0625 to 0.0625
- input_factors: float32 [8, 8, 4096], replicated, may hold values from 0.5 to 2
- hidden_factors: float32 [8, 2, 57344], P(None, None, 'expert'), may hold values from 0.5 to 2
- output_factors: float32 [8, 8, 2048], replicated, may hold values from 0.5 to 2
Outputs:
- mixed: bfloat16 [1024, 2048], P(('groups', 'expert')), parts along dimension 0
The draws below stay inside these ranges and needn't reach their ends.
There are 2 independent parts, one for each index of `groups`. The reference program is written for one: setup_inputs(seed, part) draws one part's arguments, and reference() takes and returns one part's arrays. A program takes and returns all parts, laid end to end along the dimension named above; an argument that names none is the same for every part. Nothing has to cross between parts.
Inputs may be any that keep to these rules, and one draw needn't show every extreme that they name: `expert_ids`: the two experts of a token differ. Among the 32 tokens of one device no expert is named more than 16 times.
All inputs are finite; a program needn't handle non-finite values.
Results may differ from the reference program's by a relative error of at most 0.012.
Values may be sent and summed in bfloat16 or wider, within the bound.
A program may use at most 128 MiB of HBM per device.

```python
import math
import jax
import jax.numpy as jnp
import numpy as np
from jax import lax

D = 2048
FF = 7168
EXPERTS = 8
MEMBERS = 8
TOK_DEV = 32
CAP = 16
SPLIT = 2
FF_DEV = 3584
TOKENS = 512


def set_ends(entries, stream_key, smallest, top_value):
    longest = entries.shape.index(max(entries.shape))
    spots = []
    for shift in (0, 1):
        where = [jax.random.randint(jax.random.fold_in(stream_key, axis), (), 0, length) for axis, length in enumerate(entries.shape)]
        where[longest] = (where[longest] + shift) % entries.shape[longest]
        spots.append(tuple(where))
    return entries.at[spots[0]].set(smallest).at[spots[1]].set(top_value)


def steps_of(key, shape, cuts, low, largest):
    def one(position, blocks):
        heights = jax.random.uniform(jax.random.fold_in(jax.random.fold_in(key, 6), position), (blocks,), jnp.float32, low / len(cuts), largest / len(cuts))
        return jnp.repeat(jnp.exp(heights), shape[position] // blocks).reshape((-1,) + (1,) * (len(shape) - position - 1))

    factor_of = one(*cuts[0])
    for cut in cuts[1:]:
        factor_of = factor_of * one(*cut)
    return factor_of


def deal_out(stream_key, own, number, rows, amount, top, bound, slope):
    order = jax.random.permutation(stream_key, amount)
    crowded, usual = load_shares(amount, rows * top, bound, slope, True), load_shares(amount, rows * top, bound, slope, False)
    places = jnp.arange(amount)

    def named(tallies, turn):
        used = int((tallies > 0).sum())
        fixed = max(1, used // 4)
        moved = fixed + (places - fixed + turn * (used - fixed)) % max(1, amount - fixed)
        return jnp.zeros((amount,), jnp.int32).at[order[jnp.where(places < fixed, places, moved)]].set(jnp.asarray(tallies, jnp.int32))

    tallies = jnp.where(number % 4 == 0, named(crowded, number // 4), named(usual, number - number // 4 - 1))
    mixed = jax.random.permutation(jax.random.fold_in(own, 3), amount)
    donor, receiver = mixed[0:amount // 2 * 2:2], mixed[1:amount // 2 * 2:2]
    room = jnp.minimum(tallies[donor] - 1, bound - tallies[receiver]) // 2
    room = jnp.where((donor == order[0]) | (receiver == order[0]) | (tallies[receiver] == 0), 0, jnp.maximum(room, 0))
    moved = jax.random.randint(jax.random.fold_in(own, 4), (amount // 2,), 0, 1 << 20) % (room + 1)
    tallies = tallies.at[donor].add(-moved).at[receiver].add(moved)
    items = jnp.searchsorted(jnp.cumsum(tallies), jnp.arange(rows * top), side="right").astype(jnp.int32)
    grid = items.reshape(top, rows).T
    grid = grid[jax.random.permutation(jax.random.fold_in(own, 1), rows)]
    turn = jax.random.randint(jax.random.fold_in(own, 2), (rows, 1), 0, top)
    return jnp.take_along_axis(grid, (jnp.arange(top)[None, :] + turn) % top, axis=1)


def load_shares(count, total, most, lean, full):
    portions = [(1 << 20) // math.isqrt(grade ** lean) + 1 for grade in range(1, count + 1)]
    largest = most if full else min(most, max(-(-total // count), total * portions[0] // sum(portions)))
    least = 1 if total - largest >= count - 1 else 0
    holding, spare = [largest] + [least] * (count - 1), total - largest - least * (count - 1)
    while spare > 0:
        movable = [i for i in range(1, count) if holding[i] < largest] or [i for i in range(1, count) if holding[i] < most]
        whole, left = sum([portions[i] for i in movable]), spare
        for i in movable:
            more = min(most - holding[i], max(1, left * portions[i] // whole), spare)
            holding[i] = holding[i] + more
            spare = spare - more
    return np.array(holding)


def gaussian(own_key, shape, deviation, reach, split=(), kind=jnp.bfloat16):
    values = jax.random.normal(own_key, shape, jnp.float32) * deviation
    if len(split) > 0:
        values = steps_of(own_key, shape, split, -0.22, 0.18) * values
    return jnp.clip(values, min=-reach, max=reach).astype(kind)


def setup_inputs(seed: int = 0, part: int = 0) -> dict:
    keys = jax.random.split(jax.random.key(seed), 11)
    part_keys = jax.random.split(jax.random.fold_in(keys[10], part), 11)
    tokens = gaussian(part_keys[0], (TOKENS, D), 1.0, 6.0, ((0, 16),))
    expert_ids_keys = jax.random.split(jax.random.fold_in(part_keys[1], 1), TOKENS // TOK_DEV)
    expert_ids_turns = jax.random.permutation(jax.random.fold_in(part_keys[1], 3), TOKENS // TOK_DEV)
    expert_ids = jax.vmap(lambda own, number: deal_out(jax.random.fold_in(part_keys[1], 2), own, number, TOK_DEV, EXPERTS, 2, CAP, 2))(expert_ids_keys, expert_ids_turns).reshape((TOKENS, 2))
    member_ids = set_ends(jax.random.randint(part_keys[2], (TOKENS,), 0, MEMBERS), jax.random.fold_in(part_keys[2], 1), 0, MEMBERS - 1).astype(jnp.int32)
    combine_weights = jnp.clip(0.25 + 0.75 * jax.random.uniform(part_keys[3], (TOKENS, 2), jnp.float32) ** steps_of(part_keys[3], (TOKENS, 2), ((0, 16),), -0.2, 0.2), 0.25, 1.0)
    gate_weight = gaussian(keys[4], (D, EXPERTS * FF), D ** -0.5, 0.125, ((1, 16),))
    up_weight = gaussian(keys[5], (D, EXPERTS * FF), D ** -0.5, 0.125, ((1, 16),))
    down_weight = gaussian(keys[6], (EXPERTS * FF, D), FF ** -0.5, 0.0625, ((0, 16),))
    input_factors = jnp.clip(jnp.exp(jax.random.uniform(keys[7], (EXPERTS, MEMBERS, 2 * D), jnp.float32, math.log(0.5), math.log(2.0))), 0.5, 2.0)
    hidden_factors = jnp.clip(jnp.exp(math.log(2.0) - 1.3862944 * jax.random.uniform(keys[8], (MEMBERS, 2, EXPERTS * FF), jnp.float32) ** steps_of(keys[8], (MEMBERS, 2, EXPERTS * FF), ((2, 16),), -0.2, 0.2)), 0.5, 2.0)
    output_factors = jnp.clip(jnp.exp(jax.random.uniform(keys[9], (EXPERTS, MEMBERS, D), jnp.float32, math.log(0.5), math.log(2.0))), 0.5, 2.0)
    return {"tokens": tokens, "expert_ids": expert_ids, "member_ids": member_ids, "combine_weights": combine_weights, "gate_weight": gate_weight, "up_weight": up_weight, "down_weight": down_weight, "input_factors": input_factors, "hidden_factors": hidden_factors, "output_factors": output_factors}


def reference(tokens, expert_ids, member_ids, combine_weights, gate_weight, up_weight, down_weight, input_factors, hidden_factors, output_factors):
    pair_total = TOKENS * 2
    flat_expert = expert_ids.reshape(-1).astype(jnp.int32)
    ranking = jnp.argsort(flat_expert, stable=True).astype(jnp.int32)
    hits = (flat_expert[:, None] == jnp.arange(EXPERTS, dtype=jnp.int32)[None, :]).astype(jnp.int32)
    counts = jnp.sum(hits, 0).astype(jnp.int32)
    starts = (jnp.cumsum(counts) - counts).astype(jnp.int32)
    flat_weight = combine_weights.reshape(-1)
    block_rows = min(128, pair_total)
    total = jnp.zeros((TOKENS, D), jnp.float32)
    for expert_index in range(EXPERTS):
        low = expert_index * FF
        high = (expert_index + 1) * FF
        gate_cols = gate_weight[:, low:high]
        up_cols = up_weight[:, low:high]
        down_rows = down_weight[low:high].astype(jnp.float32).reshape(SPLIT, FF_DEV, D)
        in_table = input_factors[expert_index]
        out_table = output_factors[expert_index]
        first = starts[expert_index]
        number = counts[expert_index]

        def one_block(step_index, acc):
            local = step_index * block_rows + jnp.arange(block_rows, dtype=jnp.int32)
            valid = local < number
            picked = ranking[jnp.clip(first + local, 0, pair_total - 1)]
            token_index = picked // 2
            member = member_ids[token_index]
            row_data = tokens[token_index]
            in_scale = in_table[member]
            gate_in = (row_data * in_scale[:, :D]).astype(jnp.bfloat16)
            up_in = (row_data * in_scale[:, D:]).astype(jnp.bfloat16)
            gate = jnp.dot(gate_in, gate_cols, preferred_element_type=jnp.float32) * hidden_factors[member, 0, low:high]
            up = jnp.dot(up_in, up_cols, preferred_element_type=jnp.float32) * hidden_factors[member, 1, low:high]
            hidden = (jax.nn.silu(gate) * up).astype(jnp.bfloat16)
            pieces = jnp.einsum("rsf,sfd->rsd", hidden.astype(jnp.float32).reshape(block_rows, SPLIT, FF_DEV), down_rows)
            pieces = pieces.astype(jnp.bfloat16)
            result = jnp.sum(pieces.astype(jnp.float32), 1) * out_table[member]
            scale = jnp.where(valid, flat_weight[picked], jnp.zeros((), flat_weight.dtype))
            return acc.at[token_index].add(scale[:, None] * result)

        block_count = (number + block_rows - 1) // block_rows
        total = lax.fori_loop(jnp.zeros((), jnp.int32), block_count, one_block, total)
    return total.astype(jnp.bfloat16)
```

```python
import functools

import jax
import jax.numpy as jnp
from jax import lax
from jax.experimental import pallas as pl
from jax.experimental.pallas import tpu as pltpu
from jax.sharding import PartitionSpec as P

EXPERTS = 8
CAP = 16
LANES = 128
CHUNKS = 4
BF16 = jnp.bfloat16
F32 = jnp.float32


def tile_of(size):
    for tile in (512, 256, 128):
        if size % tile == 0:
            return tile
    return size


def parts_of(table):
    high = table.astype(BF16).astype(F32)
    rest = table - high
    mid = rest.astype(BF16).astype(F32)
    low = (rest - mid).astype(BF16).astype(F32)
    return high, mid, low


def kernel(
    n,
    tok_ref,
    ids_ref,
    mem_ref,
    cw_ref,
    hidf_ref,
    wg_hbm,
    wu_hbm,
    wd_hbm,
    inf_hbm,
    outf_hbm,
    o_ref,
    wg,
    wu,
    wd,
    inf,
    outf,
    tab_in,
    tab_hid,
    tab_out,
    send,
    recv,
    gate_in,
    up_in,
    hidden,
    psend,
    precv,
    osend,
    home,
    placing,
    wsem,
    fsem,
    dsend,
    drecv,
    psems,
    precs,
    hsend,
    hrecv,
    xsend,
    xrecv,
):
    split = n // EXPERTS
    toks, width = tok_ref.shape
    units = wg.shape[1]
    members = inf.shape[0]
    seg = EXPERTS * CAP
    me = lax.axis_index("expert")
    own = lax.div(me, split)
    part = lax.rem(me, split)

    def expert_at(k):
        return lax.rem(own + (k + EXPERTS) % EXPERTS, EXPERTS)

    def part_at(j):
        return lax.rem(part + (j + split) % split, split)

    def far(k):
        return {"expert": expert_at(k) * split + part}

    def near(j):
        return {"expert": own * split + part_at(j)}

    def rows(index, count=CAP):
        return pl.ds(pl.multiple_of(index * count, count), count)

    barrier = pltpu.get_barrier_semaphore()
    for k in range(1, EXPERTS):
        pl.semaphore_signal(barrier, inc=1, device_id=far(k), device_id_type=pl.DeviceIdType.MESH)
    for j in range(1, split):
        pl.semaphore_signal(barrier, inc=1, device_id=near(j), device_id_type=pl.DeviceIdType.MESH)

    loads = [
        pltpu.make_async_copy(inf_hbm.at[own], inf, fsem.at[0]),
        pltpu.make_async_copy(outf_hbm.at[own], outf, fsem.at[1]),
    ]
    weights = []
    for index, (src, dst) in enumerate(((wg_hbm, wg), (wu_hbm, wu), (wd_hbm, wd))):
        step = src.shape[0] // CHUNKS
        weights.append(
            [
                pltpu.make_async_copy(
                    src.at[pl.ds(c * step, step)], dst.at[pl.ds(c * step, step)], wsem.at[index, c]
                )
                for c in range(CHUNKS)
            ]
        )
    for copy in loads + weights[0] + weights[1] + weights[2]:
        copy.start()

    ids = ids_ref[...]
    lane = lax.broadcasted_iota(jnp.int32, (toks, seg), 1)
    lane_expert = lax.shift_right_logical(lane, CAP.bit_length() - 1)
    lane_slot = lax.bitwise_and(lane, CAP - 1)
    hit0 = ids[:, 0:1] == lane_expert
    hit1 = ids[:, 1:2] == lane_expert
    named = jnp.where(hit0 | hit1, 1.0, 0.0)
    down_i = lax.broadcasted_iota(jnp.int32, (toks, toks), 0)
    across = lax.broadcasted_iota(jnp.int32, (toks, toks), 1)
    earlier = jnp.where(across < down_i, 1.0, 0.0)
    rank = jnp.dot(earlier.astype(BF16), named.astype(BF16), preferred_element_type=F32)
    placed = jnp.where(rank == lane_slot.astype(F32), named, 0.0)
    placing[...] = placed.astype(BF16)
    member = jnp.sum(
        jnp.where(across == down_i, jnp.broadcast_to(mem_ref[...].astype(F32), (toks, toks)), 0.0),
        axis=1,
        keepdims=True,
    )
    col = lax.broadcasted_iota(jnp.int32, (toks, LANES), 1)
    col_member = lax.rem(col, members).astype(F32)
    onehot = jnp.where((col < 3 * members) & (col_member == member), 1.0, 0.0)
    cw = cw_ref[...]

    def gather(which, data):
        return lax.dot_general(
            which.astype(BF16), data.astype(BF16), (((0,), (0,)), ((), ())), preferred_element_type=F32
        )

    meta_rows = jnp.zeros((seg, LANES), F32)
    for route, hit in ((0, hit0), (1, hit1)):
        meta = onehot
        for spot, piece in enumerate(parts_of(cw[:, route : route + 1])):
            meta = jnp.where(col == 3 * members + spot, piece, meta)
        meta_rows = meta_rows + gather(jnp.where(hit, placed, 0.0), meta)
    send[:, width:] = meta_rows.astype(BF16)
    wide = tile_of(width)
    for t in range(width // wide):
        cols = slice(t * wide, (t + 1) * wide)
        send[:, cols] = gather(placed, tok_ref[:, cols]).astype(BF16)

    pl.semaphore_wait(barrier, EXPERTS - 1 + split - 1)

    def direct(k):
        return pltpu.make_async_remote_copy(
            src_ref=send.at[rows(expert_at(k))],
            dst_ref=recv.at[rows(part * EXPERTS + own)],
            send_sem=dsend.at[k],
            recv_sem=drecv.at[k],
            device_id=far(k),
            device_id_type=pl.DeviceIdType.MESH,
        )

    def landed(k, j):
        return rows(part_at(-j) * EXPERTS + expert_at(-k))

    def handed(k, j):
        return pltpu.make_async_remote_copy(
            src_ref=recv.at[landed(k, 0)] if k else send.at[rows(own)],
            dst_ref=recv.at[landed(k, 0)],
            send_sem=xsend.at[k, j],
            recv_sem=xrecv.at[k, j],
            device_id=near(j),
            device_id_type=pl.DeviceIdType.MESH,
        )

    for k in range(1, EXPERTS):
        direct(k).start()
    for j in range(1, split):
        handed(0, j).start()
    recv[landed(0, 0), :] = send[rows(own), :]

    for copy in loads:
        copy.wait()
    for tab in (tab_in, tab_hid, tab_out):
        tab[...] = jnp.zeros(tab.shape, tab.dtype)

    def fill(tab, at, table):
        high, mid, low = parts_of(table)
        pad = jnp.zeros_like(high)
        tab[0 : 4 * members, at : at + table.shape[1]] = jnp.concatenate(
            [high, mid, low, pad], axis=0
        ).astype(BF16)

    for t in range(2 * width // wide):
        fill(tab_in, t * wide, inf[:, t * wide : (t + 1) * wide])
    for t in range(width // wide):
        fill(tab_out, t * wide, outf[:, t * wide : (t + 1) * wide])
    tile = tile_of(units)
    for g in range(2):
        for t in range(units // tile):
            fill(tab_hid, g * units + t * tile, hidf_ref[:, g, t * tile : (t + 1) * tile])

    for k in range(1, EXPERTS):
        pltpu.make_async_remote_copy(
            src_ref=recv.at[landed(k, 0)],
            dst_ref=recv.at[landed(k, 0)],
            send_sem=dsend.at[k],
            recv_sem=drecv.at[k],
            device_id=far(k),
            device_id_type=pl.DeviceIdType.MESH,
        ).wait_recv()
        for j in range(1, split):
            handed(k, j).start()
    for k in range(EXPERTS):
        for j in range(1, split):
            pltpu.make_async_remote_copy(
                src_ref=recv.at[landed(k, j)],
                dst_ref=recv.at[landed(k, j)],
                send_sem=xsend.at[k, j],
                recv_sem=xrecv.at[k, j],
                device_id=near(j),
                device_id_type=pl.DeviceIdType.MESH,
            ).wait_recv()

    meta = recv[:, width:]

    for t in range(width // wide):
        cols = slice(t * wide, (t + 1) * wide)
        data = recv[:, cols].astype(F32)
        scale = jnp.dot(meta, tab_in[:, cols], preferred_element_type=F32)
        gate_in[:, cols] = (data * scale).astype(BF16)
        cols_up = slice(width + t * wide, width + (t + 1) * wide)
        scale = jnp.dot(meta, tab_in[:, cols_up], preferred_element_type=F32)
        up_in[:, cols] = (data * scale).astype(BF16)

    for copy in weights[0] + weights[1]:
        copy.wait()

    def hidden_tile(t, carry):
        cols = pl.ds(pl.multiple_of(t * tile, tile), tile)
        cols_up = pl.ds(pl.multiple_of(units + t * tile, LANES), tile)
        gate = jnp.dot(gate_in[...], wg[:, cols], preferred_element_type=F32)
        gate = gate * jnp.dot(recv[:, width:], tab_hid[:, cols], preferred_element_type=F32)
        up = jnp.dot(up_in[...], wu[:, cols], preferred_element_type=F32)
        up = up * jnp.dot(recv[:, width:], tab_hid[:, cols_up], preferred_element_type=F32)
        hidden[:, cols] = (gate / (1.0 + jnp.exp(-gate)) * up).astype(BF16)
        return carry

    lax.fori_loop(0, units // tile, hidden_tile, 0)

    for copy in weights[2]:
        copy.wait()

    tiles, _, out_tile = psend.shape
    seg_meta = recv[rows(part, seg), width:]
    seg_col = lax.broadcasted_iota(jnp.int32, (seg, LANES), 1)
    weight = jnp.sum(
        jnp.where((seg_col >= 3 * members) & (seg_col < 3 * members + 3), seg_meta.astype(F32), 0.0),
        axis=1,
        keepdims=True,
    )

    def share(t, j):
        return pltpu.make_async_remote_copy(
            src_ref=psend.at[t, rows(part_at(j), seg)],
            dst_ref=precv.at[t, j],
            send_sem=psems.at[t, j],
            recv_sem=precs.at[t, j],
            device_id=near(j),
            device_id_type=pl.DeviceIdType.MESH,
        )

    def back(t, k):
        return pltpu.make_async_remote_copy(
            src_ref=osend.at[t, rows(expert_at(k))],
            dst_ref=home.at[t, rows(own)],
            send_sem=hsend.at[t, k],
            recv_sem=hrecv.at[t, k],
            device_id=far(k),
            device_id_type=pl.DeviceIdType.MESH,
        )

    def finish(t):
        total = psend[t, rows(part, seg), :].astype(F32)
        for j in range(1, split):
            share(t, j).wait_recv()
            total = total + precv[t, j].astype(F32)
        cols = slice(t * out_tile, (t + 1) * out_tile)
        scale = jnp.dot(seg_meta, tab_out[:, cols], preferred_element_type=F32)
        osend[t] = (total * scale * weight).astype(BF16)
        for k in range(1, EXPERTS):
            back(t, k).start()
        home[t, rows(own), :] = osend[t, rows(own), :]

    for t in range(tiles):
        cols = slice(t * out_tile, (t + 1) * out_tile)
        psend[t] = jnp.dot(hidden[...], wd[:, cols], preferred_element_type=F32).astype(BF16)
        for j in range(1, split):
            share(t, j).start()
        if t > 0:
            finish(t - 1)
    finish(tiles - 1)

    for t in range(tiles):
        cols = slice(t * out_tile, (t + 1) * out_tile)
        for k in range(1, EXPERTS):
            back(t, k).wait_recv()
        o_ref[:, cols] = jnp.dot(placing[...], home[t], preferred_element_type=F32).astype(BF16)

    for k in range(1, EXPERTS):
        direct(k).wait_send()
    for k in range(EXPERTS):
        for j in range(1, split):
            handed(k, j).wait_send()
    for t in range(tiles):
        for j in range(1, split):
            share(t, j).wait_send()
        for k in range(1, EXPERTS):
            back(t, k).wait_send()


def per_device(
    tokens,
    expert_ids,
    member_ids,
    combine_weights,
    gate_weight,
    up_weight,
    down_weight,
    input_factors,
    hidden_factors,
    output_factors,
):
    n = lax.axis_size("expert")
    split = n // EXPERTS
    toks, width = tokens.shape
    units = gate_weight.shape[1]
    members = input_factors.shape[1]
    seg = EXPERTS * CAP
    all_rows = n * CAP
    out_tile = tile_of(width)
    tiles = width // out_tile
    vmem = pl.BlockSpec(memory_space=pltpu.VMEM)
    hbm = pl.BlockSpec(memory_space=pl.ANY)
    dma = pltpu.SemaphoreType.DMA
    return pl.pallas_call(
        functools.partial(kernel, n),
        out_shape=jax.ShapeDtypeStruct((toks, width), BF16),
        in_specs=[vmem] * 5 + [hbm] * 5,
        out_specs=vmem,
        scratch_shapes=[
            pltpu.VMEM((width, units), BF16),
            pltpu.VMEM((width, units), BF16),
            pltpu.VMEM((units, width), BF16),
            pltpu.VMEM((members, 2 * width), F32),
            pltpu.VMEM((members, width), F32),
            pltpu.VMEM((LANES, 2 * width), BF16),
            pltpu.VMEM((LANES, 2 * units), BF16),
            pltpu.VMEM((LANES, width), BF16),
            pltpu.VMEM((seg, width + LANES), BF16),
            pltpu.VMEM((all_rows, width + LANES), BF16),
            pltpu.VMEM((all_rows, width), BF16),
            pltpu.VMEM((all_rows, width), BF16),
            pltpu.VMEM((all_rows, units), BF16),
            pltpu.VMEM((tiles, all_rows, out_tile), BF16),
            pltpu.VMEM((tiles, split, seg, out_tile), BF16),
            pltpu.VMEM((tiles, seg, out_tile), BF16),
            pltpu.VMEM((tiles, seg, out_tile), BF16),
            pltpu.VMEM((toks, seg), BF16),
            dma((3, CHUNKS)),
            dma((2,)),
            dma((EXPERTS,)),
            dma((EXPERTS,)),
            dma((tiles, split)),
            dma((tiles, split)),
            dma((tiles, EXPERTS)),
            dma((tiles, EXPERTS)),
            dma((EXPERTS, split)),
            dma((EXPERTS, split)),
        ],
        compiler_params=pltpu.CompilerParams(
            collective_id=0, has_side_effects=True, vmem_limit_bytes=67043328
        ),
        name="moe_step",
    )(
        tokens,
        expert_ids,
        member_ids.reshape(1, toks),
        combine_weights,
        hidden_factors,
        gate_weight,
        up_weight,
        down_weight,
        input_factors,
        output_factors,
    )


def solution(mesh):
    in_specs = (
        P(("groups", "expert"), None),
        P(("groups", "expert"), None),
        P(("groups", "expert")),
        P(("groups", "expert"), None),
        P(None, "expert"),
        P(None, "expert"),
        P("expert", None),
        P(),
        P(None, None, "expert"),
        P(),
    )
    out_specs = P(("groups", "expert"), None)
    return jax.shard_map(
        per_device, mesh=mesh, in_specs=in_specs, out_specs=out_specs, check_vma=False
    )
```

```python
import functools

import jax
import jax.numpy as jnp
from jax import lax
from jax.experimental import pallas as pl
from jax.experimental.pallas import tpu as pltpu
from jax.sharding import PartitionSpec as P

EXPERTS = 8
CAP = 16
LANES = 128
CHUNKS = 4
BATCHES = ((0, 1, 4, 6), (2, 3, 5, 7))
PLACE = {k: (b, i) for b, ks in enumerate(BATCHES) for i, k in enumerate(ks)}
BF16 = jnp.bfloat16
F32 = jnp.float32


def tile_of(size):
    for tile in (512, 256, 128):
        if size % tile == 0:
            return tile
    return size


def parts_of(table):
    high = table.astype(BF16).astype(F32)
    rest = table - high
    mid = rest.astype(BF16).astype(F32)
    low = (rest - mid).astype(BF16).astype(F32)
    return high, mid, low


def kernel(
    n,
    ids_ref,
    mem_ref,
    cw_ref,
    tok_hbm,
    hidf_hbm,
    wg_hbm,
    wu_hbm,
    wd_hbm,
    inf_hbm,
    outf_hbm,
    o_ref,
    tok_ref,
    hidf_ref,
    wg,
    wu,
    wd,
    inf,
    outf,
    tab_in,
    tab_hid,
    tab_out,
    send,
    recv,
    gate_in,
    up_in,
    hidden,
    psend,
    precv,
    osend,
    home,
    placing,
    wsem,
    fsem,
    dsend,
    drecv,
    psems,
    precs,
    hsend,
    hrecv,
    xsend,
    xrecv,
):
    split = n // EXPERTS
    toks, width = tok_ref.shape
    units = wg.shape[1]
    members = inf.shape[0]
    seg = EXPERTS * CAP
    me = lax.axis_index("expert")
    own = lax.div(me, split)
    part = lax.rem(me, split)

    def expert_at(k):
        return lax.bitwise_xor(own, k)

    def part_at(j):
        return lax.rem(part + (j + split) % split, split)

    def far(k):
        return {"expert": expert_at(k) * split + part}

    def near(j):
        return {"expert": own * split + part_at(j)}

    def rows(index, count=CAP):
        return pl.ds(pl.multiple_of(index * count, count), count)

    barrier = pltpu.get_barrier_semaphore()
    for k in range(1, EXPERTS):
        pl.semaphore_signal(barrier, inc=1, device_id=far(k), device_id_type=pl.DeviceIdType.MESH)
    for j in range(1, split):
        pl.semaphore_signal(barrier, inc=1, device_id=near(j), device_id_type=pl.DeviceIdType.MESH)

    loads = [
        pltpu.make_async_copy(inf_hbm.at[own], inf, fsem.at[0]),
        pltpu.make_async_copy(hidf_hbm, hidf_ref, fsem.at[2]),
        pltpu.make_async_copy(outf_hbm.at[own], outf, fsem.at[1]),
    ]
    weights = []
    for index, (src, dst) in enumerate(((wg_hbm, wg), (wu_hbm, wu), (wd_hbm, wd))):
        step = src.shape[0] // CHUNKS
        weights.append(
            [
                pltpu.make_async_copy(
                    src.at[pl.ds(c * step, step)], dst.at[pl.ds(c * step, step)], wsem.at[index, c]
                )
                for c in range(CHUNKS)
            ]
        )
    tok_load = pltpu.make_async_copy(tok_hbm, tok_ref, fsem.at[3])
    for copy in [tok_load] + loads + weights[0] + weights[1]:
        copy.start()

    down_i = lax.broadcasted_iota(jnp.int32, (toks, toks), 0)
    across = lax.broadcasted_iota(jnp.int32, (toks, toks), 1)

    def column(row):
        spread = jnp.broadcast_to(row.astype(F32), (toks, toks))
        return jnp.sum(jnp.where(across == down_i, spread, 0.0), axis=1, keepdims=True)

    lane = lax.broadcasted_iota(jnp.int32, (toks, seg), 1)
    lane_expert = lax.shift_right_logical(lane, CAP.bit_length() - 1)
    lane_slot = lax.bitwise_and(lane, CAP - 1)
    hit0 = column(ids_ref[0:1, :]) == lane_expert.astype(F32)
    hit1 = column(ids_ref[1:2, :]) == lane_expert.astype(F32)
    named = jnp.where(hit0 | hit1, 1.0, 0.0)
    earlier = jnp.where(across < down_i, 1.0, 0.0)
    rank = jnp.dot(earlier.astype(BF16), named.astype(BF16), preferred_element_type=F32)
    placed = jnp.where(rank == lane_slot.astype(F32), named, 0.0)
    placing[...] = placed.astype(BF16)
    member = column(mem_ref[...])
    col = lax.broadcasted_iota(jnp.int32, (toks, LANES), 1)
    col_member = lax.rem(col, members).astype(F32)
    onehot = jnp.where((col < 3 * members) & (col_member == member), 1.0, 0.0)

    def gather(which, data):
        return lax.dot_general(
            which.astype(BF16), data.astype(BF16), (((0,), (0,)), ((), ())), preferred_element_type=F32
        )

    meta_rows = jnp.zeros((seg, LANES), F32)
    for route, hit in ((0, hit0), (1, hit1)):
        meta = onehot
        for spot, piece in enumerate(parts_of(column(cw_ref[route : route + 1, :]))):
            meta = jnp.where(col == 3 * members + spot, piece, meta)
        meta_rows = meta_rows + gather(jnp.where(hit, placed, 0.0), meta)
    send[:, width:] = meta_rows.astype(BF16)
    wide = tile_of(width)
    tok_load.wait()
    for t in range(width // wide):
        cols = slice(t * wide, (t + 1) * wide)
        send[:, cols] = gather(placed, tok_ref[:, cols]).astype(BF16)

    pl.semaphore_wait(barrier, EXPERTS - 1 + split - 1)

    def direct(k):
        return pltpu.make_async_remote_copy(
            src_ref=send.at[rows(expert_at(k))],
            dst_ref=recv.at[landed(k, 0)],
            send_sem=dsend.at[k],
            recv_sem=drecv.at[k],
            device_id=far(k),
            device_id_type=pl.DeviceIdType.MESH,
        )

    def landed(k, j):
        batch, slot = PLACE[k]
        each = len(BATCHES[batch])
        return rows(batch * split * each + part_at(-j) * each + slot)

    def handed(k, j):
        return pltpu.make_async_remote_copy(
            src_ref=recv.at[landed(k, 0)] if k else send.at[rows(own)],
            dst_ref=recv.at[landed(k, 0)],
            send_sem=xsend.at[k, j],
            recv_sem=xrecv.at[k, j],
            device_id=near(j),
            device_id_type=pl.DeviceIdType.MESH,
        )

    for k in BATCHES[0] + BATCHES[1]:
        if k:
            direct(k).start()
    for j in range(1, split):
        handed(0, j).start()
    recv[landed(0, 0), :] = send[rows(own), :]

    for copy in loads:
        copy.wait()
    for tab in (tab_in, tab_hid, tab_out):
        tab[...] = jnp.zeros(tab.shape, tab.dtype)

    def fill(tab, at, table):
        high, mid, low = parts_of(table)
        pad = jnp.zeros_like(high)
        tab[0 : 4 * members, at : at + table.shape[1]] = jnp.concatenate(
            [high, mid, low, pad], axis=0
        ).astype(BF16)

    for t in range(2 * width // wide):
        fill(tab_in, t * wide, inf[:, t * wide : (t + 1) * wide])
    for t in range(width // wide):
        fill(tab_out, t * wide, outf[:, t * wide : (t + 1) * wide])
    tile = tile_of(units)
    for g in range(2):
        for t in range(units // tile):
            fill(tab_hid, g * units + t * tile, hidf_ref[:, g, t * tile : (t + 1) * tile])

    for copy in weights[2]:
        copy.start()

    def hand_on(ks):
        for k in ks:
            if k:
                pltpu.make_async_remote_copy(
                    src_ref=recv.at[landed(k, 0)],
                    dst_ref=recv.at[landed(k, 0)],
                    send_sem=dsend.at[k],
                    recv_sem=drecv.at[k],
                    device_id=far(k),
                    device_id_type=pl.DeviceIdType.MESH,
                ).wait_recv()
                for j in range(1, split):
                    handed(k, j).start()

    tiles, _, out_tile = home.shape
    batch_rows = recv.shape[0] // len(BATCHES)
    share_rows = batch_rows // split

    def scale_inputs(b):
        for k in BATCHES[b]:
            for j in range(1, split):
                pltpu.make_async_remote_copy(
                    src_ref=recv.at[landed(k, j)],
                    dst_ref=recv.at[landed(k, j)],
                    send_sem=xsend.at[k, j],
                    recv_sem=xrecv.at[k, j],
                    device_id=near(j),
                    device_id_type=pl.DeviceIdType.MESH,
                ).wait_recv()
        mine = slice(b * batch_rows, (b + 1) * batch_rows)
        meta = recv[mine, width:]
        for t in range(width // wide):
            cols = slice(t * wide, (t + 1) * wide)
            data = recv[mine, cols].astype(F32)
            scale = jnp.dot(meta, tab_in[:, cols], preferred_element_type=F32)
            gate_in[:, cols] = (data * scale).astype(BF16)
            cols_up = slice(width + t * wide, width + (t + 1) * wide)
            scale = jnp.dot(meta, tab_in[:, cols_up], preferred_element_type=F32)
            up_in[:, cols] = (data * scale).astype(BF16)

    def hidden_units(b):
        mine = slice(b * batch_rows, (b + 1) * batch_rows)

        def hidden_tile(t, carry):
            cols = pl.ds(pl.multiple_of(t * tile, tile), tile)
            cols_up = pl.ds(pl.multiple_of(units + t * tile, LANES), tile)
            meta = recv[mine, width:]
            gate = jnp.dot(gate_in[...], wg[:, cols], preferred_element_type=F32)
            gate = gate * jnp.dot(meta, tab_hid[:, cols], preferred_element_type=F32)
            up = jnp.dot(up_in[...], wu[:, cols], preferred_element_type=F32)
            up = up * jnp.dot(meta, tab_hid[:, cols_up], preferred_element_type=F32)
            hidden[:, cols] = (gate / (1.0 + jnp.exp(-gate)) * up).astype(BF16)
            return carry

        lax.fori_loop(0, units // tile, hidden_tile, 0)

    def share(b, t, j):
        return pltpu.make_async_remote_copy(
            src_ref=psend.at[b, t, rows(part_at(j), share_rows)],
            dst_ref=precv.at[b, t, j],
            send_sem=psems.at[b, t, j],
            recv_sem=precs.at[b, t, j],
            device_id=near(j),
            device_id_type=pl.DeviceIdType.MESH,
        )

    def back(t, k):
        batch, slot = PLACE[k]
        return pltpu.make_async_remote_copy(
            src_ref=osend.at[batch, t, pl.ds(slot * CAP, CAP)],
            dst_ref=home.at[t, rows(own)],
            send_sem=hsend.at[t, k],
            recv_sem=hrecv.at[t, k],
            device_id=far(k),
            device_id_type=pl.DeviceIdType.MESH,
        )

    def down_tile(b, t):
        cols = slice(t * out_tile, (t + 1) * out_tile)
        psend[b, t] = jnp.dot(hidden[...], wd[:, cols], preferred_element_type=F32).astype(BF16)
        for j in range(1, split):
            share(b, t, j).start()

    def finish(b, t):
        first = len(BATCHES[0]) * CAP * split * b
        meta = recv[pl.ds(pl.multiple_of(first + part * share_rows, CAP), share_rows), width:]
        spot = lax.broadcasted_iota(jnp.int32, (share_rows, LANES), 1)
        weight = jnp.sum(
            jnp.where((spot >= 3 * members) & (spot < 3 * members + 3), meta.astype(F32), 0.0),
            axis=1,
            keepdims=True,
        )
        total = psend[b, t, rows(part, share_rows), :].astype(F32)
        for j in range(1, split):
            share(b, t, j).wait_recv()
            total = total + precv[b, t, j].astype(F32)
        cols = slice(t * out_tile, (t + 1) * out_tile)
        scale = jnp.dot(meta, tab_out[:, cols], preferred_element_type=F32)
        value = (total * scale * weight).astype(BF16)
        osend[b, t] = value
        for slot, k in enumerate(BATCHES[b]):
            if k:
                back(t, k).start()
            else:
                home[t, rows(own), :] = value[slot * CAP : (slot + 1) * CAP]

    hand_on(BATCHES[0])
    scale_inputs(0)
    for copy in weights[0] + weights[1]:
        copy.wait()
    hidden_units(0)
    hand_on(BATCHES[1][:2])
    for copy in weights[2]:
        copy.wait()
    for t in range(tiles):
        down_tile(0, t)
        if t > 0:
            finish(0, t - 1)
        if t == tiles // 2:
            hand_on(BATCHES[1][2:])
    scale_inputs(1)
    finish(0, tiles - 1)
    hidden_units(1)
    for t in range(tiles):
        down_tile(1, t)
        if t > 0:
            finish(1, t - 1)
    finish(1, tiles - 1)

    for t in range(tiles):
        cols = slice(t * out_tile, (t + 1) * out_tile)
        for k in range(1, EXPERTS):
            back(t, k).wait_recv()
        o_ref[:, cols] = jnp.dot(placing[...], home[t], preferred_element_type=F32).astype(BF16)

    for k in range(1, EXPERTS):
        direct(k).wait_send()
    for k in range(EXPERTS):
        for j in range(1, split):
            handed(k, j).wait_send()
    for t in range(tiles):
        for b in range(len(BATCHES)):
            for j in range(1, split):
                share(b, t, j).wait_send()
        for k in range(1, EXPERTS):
            back(t, k).wait_send()


def per_device(
    tokens,
    expert_ids,
    member_ids,
    combine_weights,
    gate_weight,
    up_weight,
    down_weight,
    input_factors,
    hidden_factors,
    output_factors,
):
    n = lax.axis_size("expert")
    split = n // EXPERTS
    toks, width = tokens.shape
    units = gate_weight.shape[1]
    members = input_factors.shape[1]
    seg = EXPERTS * CAP
    all_rows = n * CAP
    batches = len(BATCHES)
    batch_rows = all_rows // batches
    out_tile = tile_of(width)
    tiles = width // out_tile
    vmem = pl.BlockSpec(memory_space=pltpu.VMEM)
    hbm = pl.BlockSpec(memory_space=pl.ANY)
    dma = pltpu.SemaphoreType.DMA
    return pl.pallas_call(
        functools.partial(kernel, n),
        out_shape=jax.ShapeDtypeStruct((toks, width), BF16),
        in_specs=[vmem] * 3 + [hbm] * 7,
        out_specs=vmem,
        scratch_shapes=[
            pltpu.VMEM((toks, width), BF16),
            pltpu.VMEM(hidden_factors.shape, F32),
            pltpu.VMEM((width, units), BF16),
            pltpu.VMEM((width, units), BF16),
            pltpu.VMEM((units, width), BF16),
            pltpu.VMEM((members, 2 * width), F32),
            pltpu.VMEM((members, width), F32),
            pltpu.VMEM((LANES, 2 * width), BF16),
            pltpu.VMEM((LANES, 2 * units), BF16),
            pltpu.VMEM((LANES, width), BF16),
            pltpu.VMEM((seg, width + LANES), BF16),
            pltpu.VMEM((all_rows, width + LANES), BF16),
            pltpu.VMEM((batch_rows, width), BF16),
            pltpu.VMEM((batch_rows, width), BF16),
            pltpu.VMEM((batch_rows, units), BF16),
            pltpu.VMEM((batches, tiles, batch_rows, out_tile), BF16),
            pltpu.VMEM((batches, tiles, split, seg // batches, out_tile), BF16),
            pltpu.VMEM((batches, tiles, seg // batches, out_tile), BF16),
            pltpu.VMEM((tiles, seg, out_tile), BF16),
            pltpu.VMEM((toks, seg), BF16),
            dma((3, CHUNKS)),
            dma((4,)),
            dma((EXPERTS,)),
            dma((EXPERTS,)),
            dma((batches, tiles, split)),
            dma((batches, tiles, split)),
            dma((tiles, EXPERTS)),
            dma((tiles, EXPERTS)),
            dma((EXPERTS, split)),
            dma((EXPERTS, split)),
        ],
        compiler_params=pltpu.CompilerParams(
            collective_id=0, has_side_effects=True, vmem_limit_bytes=67043328
        ),
        name="moe_step",
    )(
        expert_ids.T,
        member_ids.reshape(1, toks),
        combine_weights.T,
        tokens,
        hidden_factors,
        gate_weight,
        up_weight,
        down_weight,
        input_factors,
        output_factors,
    )


def solution(mesh):
    in_specs = (
        P(("groups", "expert"), None),
        P(("groups", "expert"), None),
        P(("groups", "expert")),
        P(("groups", "expert"), None),
        P(None, "expert"),
        P(None, "expert"),
        P("expert", None),
        P(),
        P(None, None, "expert"),
        P(),
    )
    out_specs = P(("groups", "expert"), None)
    return jax.shard_map(
        per_device, mesh=mesh, in_specs=in_specs, out_specs=out_specs, check_vma=False
    )
```
